32 devices in a mesh: param: 4 (over y, x), dom: 8 (over z, core).
Axes of the slice: x: 2, y: 2, z: 4, core: 2. Of those that a mesh axis runs over, the one named last changes fastest.
Arguments:
- particles: bfloat16 [128, 524288], P('dom', 'param'), may hold values from -40 to 40
- scores: bfloat16 [128, 524288], P('dom', 'param'), may hold values from -6 to 6
- basis: bfloat16 [524288, 128], P(('param', 'dom')), may hold values from -0.0078125 to 0.0078125
Outputs:
- velocity: bfloat16 [128, 524288], P('dom', 'param')
- phi: float32 [128, 128], P('dom')
The draws below stay inside these ranges and needn't reach their ends.
All inputs are finite; a program needn't handle non-finite values.
Results may differ from the reference program's by a relative error of at most 0.0049.
Values may be sent and summed in bfloat16 or wider, within the bound.
A program may use at most 128 MiB of HBM per device.

```python
import math
import jax
import jax.numpy as jnp
from jax import lax

P_SIZE = 524288
R = 128
M = 128


def draw_particles(key, part):
    first, second = jax.random.split(jax.random.fold_in(key, 11), 2)
    rows = jnp.arange(M, dtype=jnp.float32)
    jitter = jax.random.uniform(second, (M,), jnp.float32, -1.1, 1.1)
    scale = jnp.power(3.0, rows / M) * jnp.exp(jitter)
    base = jax.random.normal(first, (M, P_SIZE), jnp.float32)
    return jnp.clip(base * scale[:, None], -40.0, 40.0).astype(jnp.bfloat16)


def block_levels(own_key, dims, cuts, least, largest):
    def one(position, blocks):
        draws = jax.random.uniform(jax.random.fold_in(jax.random.fold_in(own_key, 6), position), (blocks,), jnp.float32, least / len(cuts), largest / len(cuts))
        return jnp.repeat(jnp.exp(draws), dims[position] // blocks).reshape((-1,) + (1,) * (len(dims) - position - 1))

    factor_of = one(*cuts[0])
    for cut in cuts[1:]:
        factor_of = factor_of * one(*cut)
    return factor_of


def centred(key, dims, scale, reach, shards=(), kind=jnp.bfloat16):
    loudness = block_levels(key, dims, shards, -0.22, 0.18) if shards else 1.0
    array = jax.random.normal(key, dims, jnp.float32) * scale * loudness
    return jnp.minimum(jnp.maximum(array, -reach), reach).astype(kind)


def setup_inputs(seed: int = 0) -> dict:
    streams_of = jax.random.split(jax.random.key(seed), 4)
    return {
        "particles": draw_particles(jax.random.fold_in(streams_of[3], 71), 0),
        "scores": centred(streams_of[1], (M, P_SIZE), 1.0, 6.0, ((0, 8), (1, 4))),
        "basis": centred(streams_of[2], (P_SIZE, R), P_SIZE ** -0.5, 0.0078125, ((0, 32),)),
    }


def stein_terms(own, every, every_score):
    count = every.shape[0]
    every_sq = lax.optimization_barrier(jnp.sum(every * every, axis=1))
    own_sq = lax.optimization_barrier(jnp.sum(own * own, axis=1))
    center = lax.optimization_barrier(jnp.mean(every, axis=0))
    width = 2.0 * (jnp.mean(every_sq) - jnp.sum(center * center)) / math.log(count) + 1e-06
    cross = jnp.dot(own, every.T, precision=lax.Precision.HIGHEST)
    dist = own_sq[:, None] + every_sq[None, :] - 2.0 * cross
    kern = jnp.exp(-dist / width)
    drive = jnp.dot(kern, every_score, precision=lax.Precision.HIGHEST)
    pull = jnp.dot(kern, every, precision=lax.Precision.HIGHEST)
    total = lax.optimization_barrier(jnp.sum(kern, axis=1))
    return (drive + 2.0 / width * (own * total[:, None] - pull)) / count

def reference(particles, scores, basis):
    coeffs = jnp.dot(particles, basis, preferred_element_type=jnp.float32)
    score_coeffs = jnp.dot(scores, basis, preferred_element_type=jnp.float32)
    phi = stein_terms(coeffs, coeffs, score_coeffs)
    lift = math.sqrt(P_SIZE / R)
    lifted = jnp.dot(phi.astype(jnp.bfloat16), basis.T, preferred_element_type=jnp.float32)
    velocity = (lifted * lift).astype(jnp.bfloat16)
    return (velocity, phi)
```

```python
import functools
import math

import jax
import jax.numpy as jnp
from jax import lax
from jax.experimental import pallas as pl
from jax.experimental.pallas import tpu as pltpu
from jax.sharding import PartitionSpec as P

MESH = pl.DeviceIdType.MESH
HIGH = lax.Precision.HIGHEST
NT = (((1,), (1,)), ((), ()))


def stein_rows(own, every, every_score):
    count = every.shape[0]
    square = every * every
    every_sq = lax.dot_general(
        jnp.ones((8, every.shape[1]), jnp.float32), square, NT, precision=HIGH
    )[0:1, :]
    own_sq = jnp.sum(own * own, axis=1, keepdims=True)
    center = jnp.mean(every, axis=0, keepdims=True)
    spread = jnp.sum(square) / count - jnp.sum(center * center)
    width = 2.0 * spread / math.log(count) + 1e-06
    cross = lax.dot_general(own, every, NT, precision=HIGH)
    dist = own_sq + every_sq - 2.0 * cross
    kern = jnp.exp(-dist / width)
    drive = jnp.dot(kern, every_score, precision=HIGH)
    pull = jnp.dot(kern, every, precision=HIGH)
    total = jnp.sum(kern, axis=1, keepdims=True)
    return (drive + 2.0 / width * (own * total - pull)) / count


def kernel(
    n_p, n_d, rows, depth, cr, lift,
    part_ref, score_ref, basis_ref, vel_ref, phi_ref,
    held, ps, hps, vst, hv, acc, hacc, hpart, parts, every,
    in_sem, right_send, left_send, right_recv, left_recv,
    mate_send, mate_recv, aid_send, aid_recv, hp_send, hp_recv,
    pa_send, pa_recv, ev_send, ev_recv, v_sem, hv_send, hv_recv,
):
    p = lax.axis_index("param")
    d = lax.axis_index("dom")
    z, c = d // 2, lax.rem(d, 2)
    nz = n_d // 2
    aid = nz >= 4
    steps = nz - 2 if aid else nz - 1
    kk = depth // cr
    mate = 2 * z + 1 - c
    low_help, high_help = z == 1, z == nz - 2
    helper = jnp.logical_or(low_help, high_help)
    helped = jnp.logical_or(z == 0, z == nz - 1)
    client = jnp.where(low_help, c, n_d - 2 + c)
    server = jnp.where(z == 0, 2 + c, n_d - 4 + c)
    far = jnp.where(jnp.logical_or(low_help, z == 0), nz - 1, 0)
    wide = 2 * depth

    barrier = pltpu.get_barrier_semaphore()
    for i in range(1, n_p):
        pl.semaphore_signal(barrier, inc=1, device_id=(lax.rem(p + i, n_p), d), device_id_type=MESH)
    for i in range(1, n_d):
        pl.semaphore_signal(barrier, inc=1, device_id=(p, lax.rem(d + i, n_d)), device_id_type=MESH)

    def chunk(block, k):
        return pl.ds(pl.multiple_of(block * depth + k * cr, cr), cr)

    def remote(src, dst, ss, rs, dom):
        return pltpu.make_async_remote_copy(
            src_ref=src, dst_ref=dst, send_sem=ss, recv_sem=rs,
            device_id=(p, dom), device_id_type=MESH,
        )

    own_in = pltpu.make_async_copy(
        basis_ref, held.at[pl.ds(pl.multiple_of(d * depth, depth), depth)], in_sem.at[0])
    part_in = pltpu.make_async_copy(part_ref, ps.at[pl.ds(0, rows)], in_sem.at[1])
    score_in = pltpu.make_async_copy(score_ref, ps.at[pl.ds(rows, rows)], in_sem.at[2])
    own_in.start()
    part_in.start()
    score_in.start()
    pl.semaphore_wait(barrier, n_p + n_d - 2)

    right_ok, left_ok = z < nz - 1, z > 0

    def right_copy(s, k):
        src = basis_ref.at[pl.ds(pl.multiple_of(k * cr, cr), cr)] if s == 0 else held.at[chunk(d - 2 * s, k)]
        return remote(src, held.at[chunk(d - 2 * s, k)], right_send.at[s, k], right_recv.at[s, k], d + 2)

    def left_copy(s, k):
        src = basis_ref.at[pl.ds(pl.multiple_of(k * cr, cr), cr)] if s == 0 else held.at[chunk(d + 2 * s, k)]
        return remote(src, held.at[chunk(d + 2 * s, k)], left_send.at[s, k], left_recv.at[s, k], d - 2)

    def from_left(s, k):
        at = held.at[chunk(d - 2 * s - 2, k)]
        return remote(at, at, right_send.at[s, k], right_recv.at[s, k], d - 2)

    def from_right(s, k):
        at = held.at[chunk(d + 2 * s + 2, k)]
        return remote(at, at, left_send.at[s, k], left_recv.at[s, k], d + 2)

    def mate_copy(slot, block, k):
        src = basis_ref.at[pl.ds(pl.multiple_of(k * cr, cr), cr)] if slot == 0 else held.at[chunk(block, k)]
        return remote(src, held.at[chunk(block, k)], mate_send.at[slot, k], mate_recv.at[slot, k], mate)

    def from_mate(slot, block, k):
        at = held.at[chunk(block, k)]
        return remote(at, at, mate_send.at[slot, k], mate_recv.at[slot, k], mate)

    def aid_copy(i):
        src = (part_ref, score_ref)[i].at[:, pl.ds(pl.multiple_of(far * wide, wide), wide)]
        return remote(src, hps.at[pl.ds(i * rows, rows)], aid_send.at[i], aid_recv.at[i], server)

    def aid_arrival(i):
        at = hps.at[pl.ds(i * rows, rows)]
        return remote(at, at, aid_send.at[i], aid_recv.at[i], client)

    def each_chunk(body):
        @pl.loop(0, kk)
        def _(k):
            body(k)

    def start_own(k):
        @pl.when(right_ok)
        def _():
            right_copy(0, k).start()

        @pl.when(left_ok)
        def _():
            left_copy(0, k).start()

        mate_copy(0, d, k).start()

    each_chunk(start_own)
    if aid:
        @pl.when(helped)
        def _():
            for i in range(2):
                aid_copy(i).start()

    acc[...] = jnp.zeros_like(acc)
    hacc[...] = jnp.zeros_like(hacc)
    own_in.wait()
    part_in.wait()
    score_in.wait()

    def use(block, k, last=False):
        got = held[chunk(block, k), :]
        acc[...] += jnp.dot(ps[:, chunk(block, k)], got, preferred_element_type=jnp.float32)
        if aid and last:
            @pl.when(jnp.logical_and(helper, block // 2 == far))
            def _():
                hacc[...] += jnp.dot(
                    hps[:, chunk(lax.rem(block, 2), k)], held[chunk(block, k), :],
                    preferred_element_type=jnp.float32)

    def use_own(k):
        use(d, k)
        from_mate(0, mate, k).wait_recv()
        use(mate, k)

    each_chunk(use_own)

    for s in range(steps):
        last = s == steps - 1
        has_left, has_right = z >= s + 1, z + s + 1 < nz
        if aid and last:
            @pl.when(helper)
            def _():
                for i in range(2):
                    aid_arrival(i).wait_recv()

        def arrive(k, s=s, last=last, has_left=has_left, has_right=has_right):
            @pl.when(has_left)
            def _():
                from_left(s, k).wait_recv()
                if not last:
                    @pl.when(right_ok)
                    def _():
                        right_copy(s + 1, k).start()
                mate_copy(1 + 2 * s, d - 2 * s - 2, k).start()

            @pl.when(has_right)
            def _():
                from_right(s, k).wait_recv()
                if not last:
                    @pl.when(left_ok)
                    def _():
                        left_copy(s + 1, k).start()
                mate_copy(2 + 2 * s, d + 2 * s + 2, k).start()

            @pl.when(has_left)
            def _():
                use(d - 2 * s - 2, k, last)
                from_mate(1 + 2 * s, mate - 2 * s - 2, k).wait_recv()
                use(mate - 2 * s - 2, k, last)

            @pl.when(has_right)
            def _():
                use(d + 2 * s + 2, k, last)
                from_mate(2 + 2 * s, mate + 2 * s + 2, k).wait_recv()
                use(mate + 2 * s + 2, k, last)

        each_chunk(arrive)

    if aid:
        give = remote(hacc, hpart, hp_send, hp_recv, client)
        take = remote(hacc, hpart, hp_send, hp_recv, server)

        @pl.when(helper)
        def _():
            give.start()

        @pl.when(helped)
        def _():
            take.wait_recv()
            acc[...] += hpart[...]

    parts[pl.ds(p, 1)] = acc[...][None]
    pa = []
    for i in range(1, n_p):
        copy = pltpu.make_async_remote_copy(
            src_ref=acc, dst_ref=parts.at[p], send_sem=pa_send.at[i], recv_sem=pa_recv.at[i],
            device_id=(lax.rem(p + i, n_p), d), device_id_type=MESH)
        copy.start()
        pa.append(copy)
    for i in range(1, n_p):
        src = lax.rem(p + n_p - i, n_p)
        pltpu.make_async_remote_copy(
            src_ref=acc, dst_ref=parts.at[src], send_sem=pa_send.at[i], recv_sem=pa_recv.at[i],
            device_id=(src, d), device_id_type=MESH).wait_recv()
    whole = parts[0]
    for i in range(1, n_p):
        whole = whole + parts[i]
    every[pl.ds(d, 1)] = whole[None]
    ev = []
    for i in range(1, n_d):
        copy = remote(every.at[d], every.at[d], ev_send.at[i], ev_recv.at[i], lax.rem(d + i, n_d))
        copy.start()
        ev.append(copy)
    for i in range(1, n_d):
        src = lax.rem(d + n_d - i, n_d)
        remote(every.at[src], every.at[src], ev_send.at[i], ev_recv.at[i], src).wait_recv()

    count, rank = n_d * rows, acc.shape[1]
    coeffs = every[:, 0:rows, :].reshape(count, rank)
    score_coeffs = every[:, rows:2 * rows, :].reshape(count, rank)
    mine = every[d, 0:rows, :]
    if aid:
        theirs = every[jnp.where(helper, client, d), 0:rows, :]
        phi = stein_rows(jnp.concatenate([mine, theirs], axis=0), coeffs, score_coeffs)
    else:
        phi = stein_rows(mine, coeffs, score_coeffs)
    phi_ref[...] = phi[0:rows]
    low = phi.astype(jnp.bfloat16)

    def lifted(rows_of, block, k):
        up = lax.dot_general(rows_of, held[chunk(block, k), :], NT, preferred_element_type=jnp.float32)
        return (up * lift).astype(jnp.bfloat16)

    if aid:
        def back(j, i):
            at = chunk(j, i)
            there = vel_ref.at[:, chunk(2 * far + j, i)]
            return remote(hv.at[:, at], there, hv_send.at[j, i], hv_recv.at[j, i], client)

        def back_arrival(j, i):
            there = vel_ref.at[:, chunk(2 * far + j, i)]
            return remote(hv.at[:, chunk(j, i)], there, hv_send.at[j, i], hv_recv.at[j, i], server)

        @pl.when(helper)
        def _():
            for j in range(2):
                def send_back(k, j=j):
                    hv[:, chunk(j, k)] = lifted(low[rows:2 * rows], 2 * far + j, k)
                    back(j, k).start()

                each_chunk(send_back)

    def out_copy(block, k):
        return pltpu.make_async_copy(vst.at[:, chunk(block, k)], vel_ref.at[:, chunk(block, k)], v_sem.at[block, k])

    def both(body):
        @pl.loop(0, n_d)
        def _(block):
            def one():
                each_chunk(lambda k: body(block, k))

            if aid:
                pl.when(jnp.logical_not(jnp.logical_and(helped, block // 2 == far)))(one)
            else:
                one()

    def write(block, k):
        vst[:, chunk(block, k)] = lifted(low[0:rows], block, k)
        out_copy(block, k).start()

    both(write)

    def end_own(k):
        @pl.when(right_ok)
        def _():
            right_copy(0, k).wait_send()

        @pl.when(left_ok)
        def _():
            left_copy(0, k).wait_send()

        mate_copy(0, d, k).wait_send()

    each_chunk(end_own)
    for s in range(steps):
        last = s == steps - 1
        has_left, has_right = z >= s + 1, z + s + 1 < nz

        def end(k, s=s, last=last, has_left=has_left, has_right=has_right):
            @pl.when(has_left)
            def _():
                if not last:
                    @pl.when(right_ok)
                    def _():
                        right_copy(s + 1, k).wait_send()
                mate_copy(1 + 2 * s, d - 2 * s - 2, k).wait_send()

            @pl.when(has_right)
            def _():
                if not last:
                    @pl.when(left_ok)
                    def _():
                        left_copy(s + 1, k).wait_send()
                mate_copy(2 + 2 * s, d + 2 * s + 2, k).wait_send()

        each_chunk(end)
    for copy in pa + ev:
        copy.wait_send()
    both(lambda block, k: out_copy(block, k).wait())
    if aid:
        @pl.when(helper)
        def _():
            give.wait_send()
            for j in range(2):
                each_chunk(lambda k, j=j: back(j, k).wait_send())

        @pl.when(helped)
        def _():
            for i in range(2):
                aid_copy(i).wait_send()
            for j in range(2):
                each_chunk(lambda k, j=j: back_arrival(j, k).wait_recv())


def solution(mesh):
    n_p, n_d = mesh.shape["param"], mesh.shape["dom"]

    def body(particles, scores, basis):
        rows, dims = particles.shape
        depth, rank = basis.shape
        cr = min(depth, 2048)
        kk = depth // cr
        nz = n_d // 2
        f32, bf16 = jnp.float32, jnp.bfloat16
        dma = pltpu.SemaphoreType.DMA
        anywhere = pl.BlockSpec(memory_space=pl.ANY)
        lift = math.sqrt(dims * n_p / rank)
        return pl.pallas_call(
            functools.partial(kernel, n_p, n_d, rows, depth, cr, lift),
            out_shape=(
                jax.ShapeDtypeStruct((rows, dims), bf16),
                jax.ShapeDtypeStruct((rows, rank), f32),
            ),
            in_specs=[anywhere] * 3,
            out_specs=(anywhere, pl.BlockSpec(memory_space=pltpu.VMEM)),
            scratch_shapes=[
                pltpu.VMEM((dims, rank), bf16),
                pltpu.VMEM((2 * rows, dims), bf16),
                pltpu.VMEM((2 * rows, 2 * depth), bf16),
                pltpu.VMEM((rows, dims), bf16),
                pltpu.VMEM((rows, 2 * depth), bf16),
                pltpu.VMEM((2 * rows, rank), f32),
                pltpu.VMEM((2 * rows, rank), f32),
                pltpu.VMEM((2 * rows, rank), f32),
                pltpu.VMEM((n_p, 2 * rows, rank), f32),
                pltpu.VMEM((n_d, 2 * rows, rank), f32),
                dma((3,)),
                dma((nz, kk)), dma((nz, kk)), dma((nz, kk)), dma((nz, kk)),
                dma((2 * nz, kk)), dma((2 * nz, kk)),
                dma((2,)), dma((2,)), dma, dma,
                dma((n_p,)), dma((n_p,)), dma((n_d,)), dma((n_d,)),
                dma((n_d, kk)), dma((2, kk)), dma((2, kk)),
            ],
            compiler_params=pltpu.CompilerParams(
                collective_id=0, has_side_effects=True, vmem_limit_bytes=60 * 1024 * 1024
            ),
        )(particles, scores, basis)

    in_specs = (P("dom", "param"), P("dom", "param"), P(("param", "dom"), None))
    out_specs = (P("dom", "param"), P("dom", None))
    return jax.shard_map(body, mesh=mesh, in_specs=in_specs, out_specs=out_specs, check_vma=False)
```

```python
import functools
import math

import jax
import jax.numpy as jnp
from jax import lax
from jax.experimental import pallas as pl
from jax.experimental.pallas import tpu as pltpu
from jax.sharding import PartitionSpec as P

MESH = pl.DeviceIdType.MESH
HIGH = lax.Precision.HIGHEST
NT = (((1,), (1,)), ((), ()))


def stein_rows(own, every, every_score):
    count = every.shape[0]
    square = every * every
    every_sq = lax.dot_general(
        jnp.ones((8, every.shape[1]), jnp.float32), square, NT, precision=HIGH
    )[0:1, :]
    own_sq = jnp.sum(own * own, axis=1, keepdims=True)
    center = jnp.mean(every, axis=0, keepdims=True)
    spread = jnp.sum(square) / count - jnp.sum(center * center)
    width = 2.0 * spread / math.log(count) + 1e-06
    cross = lax.dot_general(own, every, NT, precision=HIGH)
    dist = own_sq + every_sq - 2.0 * cross
    kern = jnp.exp(-dist / width)
    drive = jnp.dot(kern, every_score, precision=HIGH)
    pull = jnp.dot(kern, every, precision=HIGH)
    total = jnp.sum(kern, axis=1, keepdims=True)
    return (drive + 2.0 / width * (own * total - pull)) / count


def kernel(
    n_p, n_d, rows, depth, cr, lift,
    part_ref, score_ref, basis_ref, vel_ref, phi_ref,
    held, ps, hps, vst, hv, acc, hacc, hpart, parts, every,
    in_sem, right_send, left_send, right_recv, left_recv,
    mate_send, mate_recv, aid_send, aid_recv, hp_send, hp_recv,
    pa_send, pa_recv, ev_send, ev_recv, v_sem, hv_send, hv_recv,
):
    p = lax.axis_index("param")
    d = lax.axis_index("dom")
    z, c = d // 2, lax.rem(d, 2)
    nz = n_d // 2
    aid = nz >= 4
    steps = nz - 2 if aid else nz - 1
    kk = depth // cr
    mate = 2 * z + 1 - c
    low_help, high_help = z == 1, z == nz - 2
    helper = jnp.logical_or(low_help, high_help)
    helped = jnp.logical_or(z == 0, z == nz - 1)
    client = jnp.where(low_help, c, n_d - 2 + c)
    server = jnp.where(z == 0, 2 + c, n_d - 4 + c)
    far = jnp.where(jnp.logical_or(low_help, z == 0), nz - 1, 0)
    wide = 2 * depth

    barrier = pltpu.get_barrier_semaphore()
    for i in range(1, n_p):
        pl.semaphore_signal(barrier, inc=1, device_id=(lax.rem(p + i, n_p), d), device_id_type=MESH)
    for i in range(1, n_d):
        pl.semaphore_signal(barrier, inc=1, device_id=(p, lax.rem(d + i, n_d)), device_id_type=MESH)

    def chunk(block, k):
        return pl.ds(pl.multiple_of(block * depth + k * cr, cr), cr)

    def remote(src, dst, ss, rs, dom):
        return pltpu.make_async_remote_copy(
            src_ref=src, dst_ref=dst, send_sem=ss, recv_sem=rs,
            device_id=(p, dom), device_id_type=MESH,
        )

    own_in = pltpu.make_async_copy(
        basis_ref, held.at[pl.ds(pl.multiple_of(d * depth, depth), depth)], in_sem.at[0])
    part_in = pltpu.make_async_copy(part_ref, ps.at[pl.ds(0, rows)], in_sem.at[1])
    score_in = pltpu.make_async_copy(score_ref, ps.at[pl.ds(rows, rows)], in_sem.at[2])
    own_in.start()
    part_in.start()
    score_in.start()
    pl.semaphore_wait(barrier, n_p + n_d - 2)

    right_ok, left_ok = z < nz - 1, z > 0

    def right_copy(s, k):
        src = basis_ref.at[pl.ds(pl.multiple_of(k * cr, cr), cr)] if s == 0 else held.at[chunk(d - 2 * s, k)]
        return remote(src, held.at[chunk(d - 2 * s, k)], right_send.at[s, k], right_recv.at[s, k], d + 2)

    def left_copy(s, k):
        src = basis_ref.at[pl.ds(pl.multiple_of(k * cr, cr), cr)] if s == 0 else held.at[chunk(d + 2 * s, k)]
        return remote(src, held.at[chunk(d + 2 * s, k)], left_send.at[s, k], left_recv.at[s, k], d - 2)

    def from_left(s, k):
        at = held.at[chunk(d - 2 * s - 2, k)]
        return remote(at, at, right_send.at[s, k], right_recv.at[s, k], d - 2)

    def from_right(s, k):
        at = held.at[chunk(d + 2 * s + 2, k)]
        return remote(at, at, left_send.at[s, k], left_recv.at[s, k], d + 2)

    def mate_copy(slot, block, k):
        src = basis_ref.at[pl.ds(pl.multiple_of(k * cr, cr), cr)] if slot == 0 else held.at[chunk(block, k)]
        return remote(src, held.at[chunk(block, k)], mate_send.at[slot, k], mate_recv.at[slot, k], mate)

    def from_mate(slot, block, k):
        at = held.at[chunk(block, k)]
        return remote(at, at, mate_send.at[slot, k], mate_recv.at[slot, k], mate)

    def aid_copy(i):
        src = (part_ref, score_ref)[i].at[:, pl.ds(pl.multiple_of(far * wide, wide), wide)]
        return remote(src, hps.at[pl.ds(i * rows, rows)], aid_send.at[i], aid_recv.at[i], server)

    def aid_arrival(i):
        at = hps.at[pl.ds(i * rows, rows)]
        return remote(at, at, aid_send.at[i], aid_recv.at[i], client)

    def each_chunk(body):
        @pl.loop(0, kk)
        def _(k):
            body(k)

    def start_own(k):
        @pl.when(right_ok)
        def _():
            right_copy(0, k).start()

        @pl.when(left_ok)
        def _():
            left_copy(0, k).start()

        mate_copy(0, d, k).start()

    each_chunk(start_own)
    acc[...] = jnp.zeros_like(acc)
    hacc[...] = jnp.zeros_like(hacc)
    own_in.wait()
    part_in.wait()
    score_in.wait()

    def use(block, k, last=False):
        got = held[chunk(block, k), :]
        acc[...] += jnp.dot(ps[:, chunk(block, k)], got, preferred_element_type=jnp.float32)
        if aid and last:
            @pl.when(jnp.logical_and(helper, block // 2 == far))
            def _():
                hacc[...] += jnp.dot(
                    hps[:, chunk(lax.rem(block, 2), k)], held[chunk(block, k), :],
                    preferred_element_type=jnp.float32)

    def use_own(k):
        use(d, k)
        from_mate(0, mate, k).wait_recv()
        use(mate, k)

    each_chunk(use_own)

    for s in range(steps):
        last = s == steps - 1
        has_left, has_right = z >= s + 1, z + s + 1 < nz
        if aid and last:
            @pl.when(helper)
            def _():
                for i in range(2):
                    aid_arrival(i).wait_recv()

        def arrive(k, s=s, last=last, has_left=has_left, has_right=has_right):
            @pl.when(has_left)
            def _():
                from_left(s, k).wait_recv()
                if not last:
                    @pl.when(right_ok)
                    def _():
                        right_copy(s + 1, k).start()
                mate_copy(1 + 2 * s, d - 2 * s - 2, k).start()

            @pl.when(has_right)
            def _():
                from_right(s, k).wait_recv()
                if not last:
                    @pl.when(left_ok)
                    def _():
                        left_copy(s + 1, k).start()
                mate_copy(2 + 2 * s, d + 2 * s + 2, k).start()

            @pl.when(has_left)
            def _():
                use(d - 2 * s - 2, k, last)
                from_mate(1 + 2 * s, mate - 2 * s - 2, k).wait_recv()
                use(mate - 2 * s - 2, k, last)

            @pl.when(has_right)
            def _():
                use(d + 2 * s + 2, k, last)
                from_mate(2 + 2 * s, mate + 2 * s + 2, k).wait_recv()
                use(mate + 2 * s + 2, k, last)

        each_chunk(arrive)
        if aid and s == 0:
            @pl.when(helped)
            def _():
                for i in range(2):
                    aid_copy(i).start()

    if aid:
        give = remote(hacc, hpart, hp_send, hp_recv, client)
        take = remote(hacc, hpart, hp_send, hp_recv, server)

        @pl.when(helper)
        def _():
            give.start()

        @pl.when(helped)
        def _():
            take.wait_recv()
            acc[...] += hpart[...]

    parts[pl.ds(p, 1)] = acc[...][None]
    pa = []
    for i in range(1, n_p):
        copy = pltpu.make_async_remote_copy(
            src_ref=acc, dst_ref=parts.at[p], send_sem=pa_send.at[i], recv_sem=pa_recv.at[i],
            device_id=(lax.rem(p + i, n_p), d), device_id_type=MESH)
        copy.start()
        pa.append(copy)
    for i in range(1, n_p):
        src = lax.rem(p + n_p - i, n_p)
        pltpu.make_async_remote_copy(
            src_ref=acc, dst_ref=parts.at[src], send_sem=pa_send.at[i], recv_sem=pa_recv.at[i],
            device_id=(src, d), device_id_type=MESH).wait_recv()
    whole = parts[0]
    for i in range(1, n_p):
        whole = whole + parts[i]
    every[pl.ds(d, 1)] = whole[None]
    ev = []
    for i in range(1, n_d):
        copy = remote(every.at[d], every.at[d], ev_send.at[i], ev_recv.at[i], lax.rem(d + i, n_d))
        copy.start()
        ev.append(copy)
    for i in range(1, n_d):
        src = lax.rem(d + n_d - i, n_d)
        remote(every.at[src], every.at[src], ev_send.at[i], ev_recv.at[i], src).wait_recv()

    count, rank = n_d * rows, acc.shape[1]
    coeffs = every[:, 0:rows, :].reshape(count, rank)
    score_coeffs = every[:, rows:2 * rows, :].reshape(count, rank)
    mine = every[d, 0:rows, :]
    if aid:
        theirs = every[jnp.where(helper, client, d), 0:rows, :]
        phi = stein_rows(jnp.concatenate([mine, theirs], axis=0), coeffs, score_coeffs)
    else:
        phi = stein_rows(mine, coeffs, score_coeffs)
    phi_ref[...] = phi[0:rows]
    low = phi.astype(jnp.bfloat16)

    half = cr // 2

    def spread(rows_of):
        blank = jnp.zeros_like(rows_of)
        upper = jnp.concatenate([rows_of, blank], axis=1)
        lower = jnp.concatenate([blank, rows_of], axis=1)
        return jnp.concatenate([upper, lower], axis=0)

    def lifted(spread_rows, block, k):
        start = pl.multiple_of(block * depth + k * cr, cr)
        first, second = held[pl.ds(start, half), :], held[pl.ds(pl.multiple_of(start + half, half), half), :]
        up = lax.dot_general(
            spread_rows, jnp.concatenate([first, second], axis=1), NT,
            preferred_element_type=jnp.float32)
        return (up * lift).astype(jnp.bfloat16)

    def halves(j, k):
        start = pl.multiple_of(j * depth + k * cr, cr)
        return pl.ds(start, half), pl.ds(pl.multiple_of(start + half, half), half)

    def out_copy(block, k):
        return pltpu.make_async_copy(vst.at[:, chunk(block, k)], vel_ref.at[:, chunk(block, k)], v_sem.at[block, k])

    def keep(up, block, k, total):
        left, right = halves(block, k)
        vst[:, left] = up[0:rows]
        vst[:, right] = up[total:total + rows]
        out_copy(block, k).start()

    if aid:
        def back(j, i):
            at = chunk(j, i)
            there = vel_ref.at[:, chunk(2 * far + j, i)]
            return remote(hv.at[:, at], there, hv_send.at[j, i], hv_recv.at[j, i], client)

        def back_arrival(j, i):
            there = vel_ref.at[:, chunk(2 * far + j, i)]
            return remote(hv.at[:, chunk(j, i)], there, hv_send.at[j, i], hv_recv.at[j, i], server)

        @pl.when(helper)
        def _():
            low_both = spread(low)
            for j in range(2):
                def send_back(k, j=j):
                    up = lifted(low_both, 2 * far + j, k)
                    left, right = halves(j, k)
                    hv[:, left] = up[rows:2 * rows]
                    hv[:, right] = up[3 * rows:4 * rows]
                    back(j, k).start()
                    keep(up, 2 * far + j, k, 2 * rows)

                each_chunk(send_back)

    def both(body, skip):
        @pl.loop(0, n_d)
        def _(block):
            def one():
                each_chunk(lambda k: body(block, k))

            if aid:
                pl.when(jnp.logical_not(jnp.logical_and(skip, block // 2 == far)))(one)
            else:
                one()

    low_own = spread(low[0:rows])

    def write(block, k):
        keep(lifted(low_own, block, k), block, k, rows)

    both(write, jnp.logical_or(helper, helped))

    def end_own(k):
        @pl.when(right_ok)
        def _():
            right_copy(0, k).wait_send()

        @pl.when(left_ok)
        def _():
            left_copy(0, k).wait_send()

        mate_copy(0, d, k).wait_send()

    each_chunk(end_own)
    for s in range(steps):
        last = s == steps - 1
        has_left, has_right = z >= s + 1, z + s + 1 < nz

        def end(k, s=s, last=last, has_left=has_left, has_right=has_right):
            @pl.when(has_left)
            def _():
                if not last:
                    @pl.when(right_ok)
                    def _():
                        right_copy(s + 1, k).wait_send()
                mate_copy(1 + 2 * s, d - 2 * s - 2, k).wait_send()

            @pl.when(has_right)
            def _():
                if not last:
                    @pl.when(left_ok)
                    def _():
                        left_copy(s + 1, k).wait_send()
                mate_copy(2 + 2 * s, d + 2 * s + 2, k).wait_send()

        each_chunk(end)
    for copy in pa + ev:
        copy.wait_send()
    both(lambda block, k: out_copy(block, k).wait(), helped)
    if aid:
        @pl.when(helper)
        def _():
            give.wait_send()
            for j in range(2):
                each_chunk(lambda k, j=j: back(j, k).wait_send())

        @pl.when(helped)
        def _():
            for i in range(2):
                aid_copy(i).wait_send()
            for j in range(2):
                each_chunk(lambda k, j=j: back_arrival(j, k).wait_recv())


def solution(mesh):
    n_p, n_d = mesh.shape["param"], mesh.shape["dom"]

    def body(particles, scores, basis):
        rows, dims = particles.shape
        depth, rank = basis.shape
        cr = min(depth, 2048)
        kk = depth // cr
        nz = n_d // 2
        f32, bf16 = jnp.float32, jnp.bfloat16
        dma = pltpu.SemaphoreType.DMA
        anywhere = pl.BlockSpec(memory_space=pl.ANY)
        lift = math.sqrt(dims * n_p / rank)
        return pl.pallas_call(
            functools.partial(kernel, n_p, n_d, rows, depth, cr, lift),
            out_shape=(
                jax.ShapeDtypeStruct((rows, dims), bf16),
                jax.ShapeDtypeStruct((rows, rank), f32),
            ),
            in_specs=[anywhere] * 3,
            out_specs=(anywhere, pl.BlockSpec(memory_space=pltpu.VMEM)),
            scratch_shapes=[
                pltpu.VMEM((dims, rank), bf16),
                pltpu.VMEM((2 * rows, dims), bf16),
                pltpu.VMEM((2 * rows, 2 * depth), bf16),
                pltpu.VMEM((rows, dims), bf16),
                pltpu.VMEM((rows, 2 * depth), bf16),
                pltpu.VMEM((2 * rows, rank), f32),
                pltpu.VMEM((2 * rows, rank), f32),
                pltpu.VMEM((2 * rows, rank), f32),
                pltpu.VMEM((n_p, 2 * rows, rank), f32),
                pltpu.VMEM((n_d, 2 * rows, rank), f32),
                dma((3,)),
                dma((nz, kk)), dma((nz, kk)), dma((nz, kk)), dma((nz, kk)),
                dma((2 * nz, kk)), dma((2 * nz, kk)),
                dma((2,)), dma((2,)), dma, dma,
                dma((n_p,)), dma((n_p,)), dma((n_d,)), dma((n_d,)),
                dma((n_d, kk)), dma((2, kk)), dma((2, kk)),
            ],
            compiler_params=pltpu.CompilerParams(
                collective_id=0, has_side_effects=True, vmem_limit_bytes=50 * 1024 * 1024
            ),
        )(particles, scores, basis)

    in_specs = (P("dom", "param"), P("dom", "param"), P(("param", "dom"), None))
    out_specs = (P("dom", "param"), P("dom", None))
    return jax.shard_map(body, mesh=mesh, in_specs=in_specs, out_specs=out_specs, check_vma=False)
```
